32 devices in a mesh: lat: 8 (over y, x, core), lon: 4 (over z).
Axes of the slice: x: 2, y: 2, z: 4, core: 2. Of those that a mesh axis runs over, the one named last changes fastest.
Arguments:
- current: bfloat16 [69, 256, 512], P(None, 'lat', 'lon')
- next_fields: bfloat16 [96, 256, 512], P(('lat', 'lon')), may hold values from -6 to 6
- reader_slot: int32 [69], replicated, may hold values from 0 to 95, as said below
- first_weight: bfloat16 [9, 256, 69], replicated, may hold values from -0.25 to 0.25
- first_bias: float32 [256], replicated, may hold values from -3 to 3
- second_weight: bfloat16 [9, 256, 256], replicated, may hold values from -0.125 to 0.125
- second_bias: float32 [256], replicated, may hold values from -3 to 3
Outputs:
- features: bfloat16 [256, 256, 512], P(None, 'lat', 'lon')
- next_tile: bfloat16 [69, 256, 512], P(None, 'lat', 'lon')
The draws below stay inside these ranges and needn't reach their ends.
Inputs may be any that keep to these rules, and one draw needn't show every extreme that they name: `reader_slot`: the 69 entries are different slots.
All inputs are finite; a program needn't handle non-finite values.
Results may differ from the reference program's by a relative error of at most 0.0053.
Values may be sent and summed in bfloat16 or wider, within the bound.
A program may use at most 128 MiB of HBM per device.

```python
import jax
import jax.numpy as jnp
from jax import lax

C = 69
HID = 256
LAT_DEV = 32
LON_DEV = 128
H = 256
W = 512
SLOTS = 96


def draw_current(key, part):
    keys = jax.random.split(jax.random.fold_in(key, 11), 7)
    profile = (jnp.arange(H, dtype=jnp.float32) / (H - 1))[None, :, None]
    rough = jax.random.uniform(keys[4], (C, 1, W), jnp.float32, 0.5, 1.5)
    slope = jax.random.uniform(keys[2], (C, 1, 1), jnp.float32, -2.0, 2.0)
    lat_tiles = H // LAT_DEV
    lon_tiles = W // LON_DEV
    tile_level = jax.random.normal(keys[5], (C, lat_tiles, 1, lon_tiles, 1), jnp.float32)
    tile_field = jnp.broadcast_to(tile_level, (C, lat_tiles, LAT_DEV, lon_tiles, LON_DEV)).reshape(C, H, W)
    half_level = jax.random.normal(keys[6], (C, 1, 2), jnp.float32)
    half_field = jnp.repeat(half_level, W // 2, axis=2)
    noise = jax.random.normal(keys[0], (C, H, W), jnp.float32)
    offset = jax.random.normal(keys[1], (C, 1, 1), jnp.float32)
    spread = 1.0 + 2.0 * profile
    tile_scale = 0.8
    values = offset + 3.0 * slope * profile + tile_scale * tile_field + half_field + spread * rough * noise
    return values.astype(jnp.bfloat16)


def draw_reader_slot(key, part):
    order = jax.random.permutation(jax.random.fold_in(key, 23), SLOTS)
    return order[:C].astype(jnp.int32)


def steps_of(rng, shape, shards, smallest, top_value):
    loudness = 1.0
    for dim, shards_of in shards:
        heights = jax.random.uniform(jax.random.fold_in(jax.random.fold_in(rng, 6), dim), (shards_of,), jnp.float32, smallest / len(shards), top_value / len(shards))
        loudness = loudness * jnp.repeat(jnp.exp(heights), shape[dim] // shards_of).reshape((-1,) + (1,) * (len(shape) - 1 - dim))
    return loudness


def scatter_about(own_key, dims, scale, most, cuts=(), held_as=jnp.bfloat16):
    level = steps_of(own_key, dims, cuts, -0.22, 0.18) if cuts else 1.0
    drawn = jax.random.normal(own_key, dims, jnp.float32) * scale * level
    return jnp.minimum(jnp.maximum(drawn, -most), most).astype(held_as)


def setup_inputs(seed: int = 0) -> dict:
    key_of = jax.random.split(jax.random.key(seed), 8)
    current = draw_current(jax.random.fold_in(key_of[7], 71), 0)
    next_fields = scatter_about(key_of[1], (SLOTS, H, W), 1.0, 6.0, ((0, 32),))
    reader_slot = draw_reader_slot(jax.random.fold_in(key_of[7], 71), 0)
    first_weight = scatter_about(key_of[3], (9, HID, C), (9 * C) ** -0.5, 0.25)
    first_bias = scatter_about(key_of[4], (HID,), 0.5, 3.0, (), jnp.float32)
    second_weight = scatter_about(key_of[5], (9, HID, HID), (9 * HID) ** -0.5, 0.125)
    second_bias = scatter_about(key_of[6], (HID,), 0.5, 3.0, (), jnp.float32)
    return {"current": current, "next_fields": next_fields, "reader_slot": reader_slot, "first_weight": first_weight, "first_bias": first_bias, "second_weight": second_weight, "second_bias": second_bias}


def conv_grid(field, weight):
    padded = jnp.pad(field.astype(jnp.float32), ((0, 0), (1, 1), (0, 0)))
    padded = jnp.concatenate([padded[:, :, -1:], padded, padded[:, :, :1]], axis=2)
    rows = field.shape[1]
    cols = field.shape[2]
    total = jnp.zeros((weight.shape[1], rows, cols), jnp.float32)
    for tap in range(9):
        shifted = padded[:, tap // 3:tap // 3 + rows, tap % 3:tap % 3 + cols]
        total = total + jnp.einsum('ok,khw->ohw', weight[tap].astype(jnp.float32), shifted)
    return total

def reference(current, next_fields, reader_slot, first_weight, first_bias, second_weight, second_bias):
    values = current.astype(jnp.float32)
    cells = values.shape[1] * values.shape[2]
    mean = lax.optimization_barrier(jnp.sum(values, axis=(1, 2))) / cells
    square = lax.optimization_barrier(jnp.sum(values * values, axis=(1, 2))) / cells
    scale = 1.0 / jnp.sqrt(square - mean * mean + 1e-05)
    normed = ((values - mean[:, None, None]) * scale[:, None, None]).astype(jnp.bfloat16)
    hidden = jax.nn.gelu(conv_grid(normed, first_weight) + first_bias[:, None, None], approximate=True).astype(jnp.bfloat16)
    features = (conv_grid(hidden, second_weight) + second_bias[:, None, None]).astype(jnp.bfloat16)
    next_tile = jnp.take(next_fields, reader_slot, axis=0)
    return (features, next_tile)
```

```python
import functools

import jax
import jax.numpy as jnp
from jax import lax
from jax.experimental import pallas as pl
from jax.experimental.pallas import tpu as pltpu
from jax.sharding import PartitionSpec as P

MESH = pl.DeviceIdType.MESH
F32 = jnp.float32
BF16 = jnp.bfloat16
LANES = 128


def gelu(v):
    return 0.5 * v * (1.0 + jnp.tanh(0.7978845608028654 * (v + 0.044715 * v * v * v)))


def kernel(
    dims, cur, nf, slot, w1, b1, w2, b2, feat, tile,
    xf, xt, cols, hcol, en, eh, xs, hs, w1s, w2s, stats, moved,
    st_send, st_recv, ha_send, ha_recv, mv_send, mv_recv, own_sem,
):
    n_lat, n_lon, chans, rows, wide, slots, hid = dims
    n = n_lat * n_lon
    kp = LANES
    cp = -(-chans // 8) * 8
    lat = lax.axis_index("lat")
    lon = lax.axis_index("lon")
    me = lat * n_lon + lon

    barrier = pltpu.get_barrier_semaphore()

    def greet(d, carry):
        t = lax.rem(me + d, n)
        pl.semaphore_signal(
            barrier, inc=1, device_id=(t // n_lon, lax.rem(t, n_lon)), device_id_type=MESH
        )
        return carry

    lax.fori_loop(1, n, greet, 0)

    xf[pl.ds(0, chans * rows), :] = cur[...].astype(F32)
    if cp > chans:
        xf[pl.ds(chans * rows, (cp - chans) * rows), :] = jnp.zeros(((cp - chans) * rows, wide), F32)

    def turn(r, carry):
        total, square = carry
        a = xf[pl.ds(r, cp, stride=rows), :]
        a = jnp.concatenate([a, jnp.zeros((kp - cp, wide), F32)], axis=0)
        t = a.T
        xt[r + 2] = t.astype(BF16)
        cols[0, pl.ds(2 * r, 1), :] = t[0:1]
        cols[0, pl.ds(2 * r + 1, 1), :] = t[1:2]
        cols[1, pl.ds(2 * r, 1), :] = t[wide - 2 : wide - 1]
        cols[1, pl.ds(2 * r + 1, 1), :] = t[wide - 1 : wide]
        parts = t.reshape(wide // 8, 8, kp)
        return total + jnp.sum(parts, axis=0), square + jnp.sum(parts * parts, axis=0)

    zero = jnp.zeros((8, kp), F32)
    total, square = lax.fori_loop(0, rows, turn, (zero, zero))
    stats[pl.ds(me, 1), 0:1, :] = jnp.sum(total, axis=0, keepdims=True)[None]
    stats[pl.ds(me, 1), 1:2, :] = jnp.sum(square, axis=0, keepdims=True)[None]

    pl.semaphore_wait(barrier, n - 1)

    def stat_copy(d, source):
        t = lax.rem(me + d, n)
        return pltpu.make_async_remote_copy(
            src_ref=stats.at[source], dst_ref=stats.at[source],
            send_sem=st_send.at[d], recv_sem=st_recv.at[d],
            device_id=(t // n_lon, lax.rem(t, n_lon)), device_id_type=MESH,
        )

    def stat_start(d, carry):
        stat_copy(d, me).start()
        return carry

    lax.fori_loop(1, n, stat_start, 0)

    north, south = lax.rem(lat + n_lat - 1, n_lat), lax.rem(lat + 1, n_lat)
    west, east = lax.rem(lon + n_lon - 1, n_lon), lax.rem(lon + 1, n_lon)
    halos = []
    for side, col_to in ((0, west), (1, east)):
        into = 1 - side
        halos.append((cols.at[side], hcol.at[into, pl.ds(8, 2 * rows)], (lat, col_to)))
        halos.append((cols.at[side, pl.ds(0, 8)], hcol.at[into, pl.ds(8 + 2 * rows, 8)], (north, col_to)))
        halos.append((cols.at[side, pl.ds(2 * rows - 8, 8)], hcol.at[into, pl.ds(0, 8)], (south, col_to)))
    halos.append((xt.at[pl.ds(2, 2)], xt.at[pl.ds(rows + 2, 2)], (north, lon)))
    halos.append((xt.at[pl.ds(rows, 2)], xt.at[pl.ds(0, 2)], (south, lon)))
    copies = [
        pltpu.make_async_remote_copy(
            src_ref=src, dst_ref=dst, send_sem=ha_send.at[i], recv_sem=ha_recv.at[i],
            device_id=where, device_id_type=MESH,
        )
        for i, (src, dst, where) in enumerate(halos)
    ]
    for copy in copies:
        copy.start()

    def field_copy(d, source):
        t = lax.rem(me + d, n)
        tl, tn = t // n_lon, lax.rem(t, n_lon)
        return pltpu.make_async_remote_copy(
            src_ref=nf.at[:, pl.ds(pl.multiple_of(tl * rows, rows), rows), pl.ds(pl.multiple_of(tn * wide, wide), wide)],
            dst_ref=moved.at[pl.ds(source * slots, slots)],
            send_sem=mv_send.at[d], recv_sem=mv_recv.at[d],
            device_id=(tl, tn), device_id_type=MESH,
        )

    def field_start(d, carry):
        field_copy(d, me).start()
        return carry

    lax.fori_loop(1, n, field_start, 0)
    own = pltpu.make_async_copy(
        nf.at[:, pl.ds(pl.multiple_of(lat * rows, rows), rows), pl.ds(pl.multiple_of(lon * wide, wide), wide)],
        moved.at[pl.ds(me * slots, slots)],
        own_sem,
    )
    own.start()

    for tap in range(9):
        w1s[pl.ds(tap * kp, kp), :] = jnp.concatenate(
            [w1[tap].astype(F32), jnp.zeros((kp - chans, hid), F32)], axis=0
        ).astype(BF16)

    def turn_weight(tap, carry):
        w2s[pl.ds(pl.multiple_of(tap * hid, hid), hid), :] = w2[tap].astype(F32).T.astype(BF16)
        return carry

    lax.fori_loop(0, 9, turn_weight, 0)

    def stat_wait(d, carry):
        copy = stat_copy(d, lax.rem(me - d + n, n))
        copy.wait_recv()
        return carry

    lax.fori_loop(1, n, stat_wait, 0)
    sums = jnp.sum(stats[...], axis=0)
    cells = n * rows * wide
    mean = sums[0:1] / cells
    scale = 1.0 / jnp.sqrt(sums[1:2] / cells - mean * mean + 1e-05)

    for copy in copies:
        copy.wait_recv()

    first = jnp.where(lat == 0, 0, -2)
    last = jnp.where(lat == n_lat - 1, rows - 1, rows + 1)
    tall = rows + 4
    step = en.shape[1]

    line = lax.broadcasted_iota(jnp.int32, (step, 1), 0) - 2
    inside = (line >= first) & (line <= last)
    en[...] = jnp.zeros_like(en)
    for side in range(2):
        mid = 2 if side == 0 else 0
        for j in range(2):
            en[3 * side + (j if side == 0 else j + 1), pl.ds(0, tall), :] = hcol[side, pl.ds(4 + j, tall, stride=2), :]
        at = 0 if side == 0 else wide - 1
        base = 0 if side == 0 else wide - 16
        en[3 * side + mid, pl.ds(2, rows), :] = cols[side, pl.ds(0 if side == 0 else 1, rows, stride=2), :]
        for p in (0, 1, rows + 2, rows + 3):
            en[3 * side + mid, pl.ds(p, 1), :] = xt[p, pl.ds(base, 16), :].astype(F32)[at - base : at - base + 1]
    for k in range(6):
        en[k] = jnp.where(inside, (en[k] - mean) * scale, 0.0)
    bias1 = b1[...]
    bias2 = b2[...]
    hline = lax.broadcasted_iota(jnp.int32, (rows + 2, 1), 0) - 1
    hinside = (hline >= first) & (hline <= last)
    for side in range(2):
        edge = jnp.concatenate([en[3 * side + k] for k in range(3)], axis=1).astype(BF16)
        z = [
            jnp.dot(edge, w1s[pl.ds(3 * a * kp, 3 * kp), :], preferred_element_type=F32)
            for a in range(3)
        ]
        h = z[0][0 : rows + 2] + z[1][1 : rows + 3] + z[2][2 : rows + 4] + bias1
        eh[side, pl.ds(0, rows + 2), :] = jnp.where(hinside, gelu(h), 0.0)

    spot = lax.broadcasted_iota(jnp.int32, (wide, 1), 0)

    def spread(x, left, right):
        lo = jnp.where(spot == 0, left, pltpu.roll(x, 1, 0))
        hi = jnp.where(spot == wide - 1, right, pltpu.roll(x, wide - 1, 0))
        return lo.astype(BF16), x.astype(BF16), hi.astype(BF16)

    def normal(p, carry):
        ok = (p - 2 >= first) & (p - 2 <= last)
        x = (xt[p].astype(F32) - mean) * scale
        x = jnp.where(ok, x, 0.0)
        three = spread(x, en[1, pl.ds(p, 1), :], en[4, pl.ds(p, 1), :])
        for k in range(3):
            xs[p, :, k * kp : (k + 1) * kp] = three[k]
        return carry

    lax.fori_loop(0, tall, normal, 0)

    def one(b, carry):
        q = 2 * b
        left = jnp.concatenate(
            [xs[pl.ds(q + a, 2)].reshape(2 * wide, 3 * kp) for a in range(3)], axis=1
        )
        h = gelu(jnp.dot(left, w1s[...], preferred_element_type=F32) + bias1)
        for k in range(2):
            ok = (q + k - 1 >= first) & (q + k - 1 <= last)
            x = jnp.where(ok, h[k * wide : (k + 1) * wide], 0.0)
            three = spread(x, eh[0, pl.ds(q + k, 1), :], eh[1, pl.ds(q + k, 1), :])
            for m in range(3):
                hs[q + k, :, m * hid : (m + 1) * hid] = three[m]
        return carry

    lax.fori_loop(0, (rows + 2) // 2, one, 0)

    def two(b, carry):
        q = 2 * b
        left = jnp.concatenate(
            [hs[pl.ds(q + a, 2)].reshape(2 * wide, 3 * hid) for a in range(3)], axis=1
        )
        out = jnp.dot(left, w2s[...], preferred_element_type=F32) + bias2
        feat[pl.ds(pl.multiple_of(q * wide, 2 * wide), 2 * wide), :] = out.astype(BF16)
        return carry

    lax.fori_loop(0, rows // 2, two, 0)

    own.wait()

    def field_wait(d, carry):
        field_copy(d, lax.rem(me - d + n, n)).wait_recv()
        return carry

    lax.fori_loop(1, n, field_wait, 0)

    def take(c, carry):
        tile[c] = moved[slot[c]]
        return carry

    lax.fori_loop(0, chans, take, 0)

    def sent(d, carry):
        stat_copy(d, me).wait_send()
        field_copy(d, me).wait_send()
        return carry

    lax.fori_loop(1, n, sent, 0)
    for copy in copies:
        copy.wait_send()


def body(current, next_fields, reader_slot, first_weight, first_bias, second_weight, second_bias):
    n_lat, n_lon = lax.axis_size("lat"), lax.axis_size("lon")
    n = n_lat * n_lon
    chans, rows, wide = current.shape
    slots = next_fields.shape[0]
    hid = first_weight.shape[1]
    kp = LANES
    cp = -(-chans // 8) * 8
    step = -(-(rows + 4) // 16) * 16
    dims = (n_lat, n_lon, chans, rows, wide, slots, hid)
    vmem = pl.BlockSpec(memory_space=pltpu.VMEM)
    features, tile = pl.pallas_call(
        functools.partial(kernel, dims),
        out_shape=(
            jax.ShapeDtypeStruct((rows * wide, hid), BF16),
            jax.ShapeDtypeStruct((chans, rows, wide), BF16),
        ),
        in_specs=[
            vmem, pl.BlockSpec(memory_space=pl.ANY), pl.BlockSpec(memory_space=pltpu.SMEM),
            vmem, vmem, vmem, vmem,
        ],
        out_specs=(vmem, vmem),
        scratch_shapes=[
            pltpu.VMEM((cp * rows, wide), F32),
            pltpu.VMEM((rows + 4, wide, kp), BF16),
            pltpu.VMEM((2, 2 * rows, kp), F32),
            pltpu.VMEM((2, 2 * rows + 16, kp), F32),
            pltpu.VMEM((6, step, kp), F32),
            pltpu.VMEM((2, step, hid), F32),
            pltpu.VMEM((rows + 4, wide, 3 * kp), BF16),
            pltpu.VMEM((rows + 2, wide, 3 * hid), BF16),
            pltpu.VMEM((9 * kp, hid), BF16),
            pltpu.VMEM((9 * hid, hid), BF16),
            pltpu.VMEM((n, 2, kp), F32),
            pltpu.VMEM((n * slots, rows, wide), BF16),
            pltpu.SemaphoreType.DMA((n,)),
            pltpu.SemaphoreType.DMA((n,)),
            pltpu.SemaphoreType.DMA((8,)),
            pltpu.SemaphoreType.DMA((8,)),
            pltpu.SemaphoreType.DMA((n,)),
            pltpu.SemaphoreType.DMA((n,)),
            pltpu.SemaphoreType.DMA,
        ],
        compiler_params=pltpu.CompilerParams(
            collective_id=0, has_side_effects=True, vmem_limit_bytes=60 * 1024 * 1024
        ),
    )(
        current.reshape(chans * rows, wide), next_fields, reader_slot,
        first_weight.transpose(0, 2, 1), first_bias[None], second_weight, second_bias[None],
    )
    return features.reshape(rows, wide, hid).transpose(2, 0, 1), tile


def solution(mesh):
    in_specs = (P(None, "lat", "lon"), P(("lat", "lon"), None, None), P(), P(), P(), P(), P())
    out_specs = (P(None, "lat", "lon"), P(None, "lat", "lon"))
    return jax.shard_map(body, mesh=mesh, in_specs=in_specs, out_specs=out_specs, check_vma=False)
```

```python
import functools

import jax
import jax.numpy as jnp
from jax import lax
from jax.experimental import pallas as pl
from jax.experimental.pallas import tpu as pltpu
from jax.sharding import PartitionSpec as P

MESH = pl.DeviceIdType.MESH
F32 = jnp.float32
BF16 = jnp.bfloat16
LANES = 128
EARLY = 4


def gelu(v):
    return 0.5 * v * (1.0 + jnp.tanh(0.7978845608028654 * (v + 0.044715 * v * v * v)))


def kernel(
    dims, cur_in, nf, slot_in, w1_in, b1_in, w2_in, b2_in, feat, tile,
    cur, w1, w2, b1, b2, slot, yf, in_sem, xf, xt, cols, hcol, en, eh, xs, hs, w1s, w2s, stats, moved,
    st_send, st_recv, ha_send, ha_recv, mv_send, mv_recv, own_sem,
):
    n_lat, n_lon, chans, rows, wide, slots, hid = dims
    n = n_lat * n_lon
    kp = LANES
    cp = -(-chans // 8) * 8
    pitch = xf.shape[1]
    xflat = xf.reshape(cp * pitch, wide)
    yflat = yf.reshape(hid * pitch, wide)
    lat = lax.axis_index("lat")
    lon = lax.axis_index("lon")
    me = lat * n_lon + lon

    loads = [
        pltpu.make_async_copy(src, dst, in_sem.at[i])
        for i, (src, dst) in enumerate(((cur_in, cur), (w1_in, w1), (w2_in, w2), (b1_in, b1), (b2_in, b2), (slot_in, slot)))
    ]
    for load in loads:
        load.start()

    barrier = pltpu.get_barrier_semaphore()

    def greet(d, carry):
        t = lax.rem(me + d, n)
        pl.semaphore_signal(
            barrier, inc=1, device_id=(t // n_lon, lax.rem(t, n_lon)), device_id_type=MESH
        )
        return carry

    lax.fori_loop(1, n, greet, 0)

    loads[0].wait()
    xf[0:chans, 0:rows, :] = cur[...].astype(F32)
    if cp > chans:
        xf[chans:cp, :, :] = jnp.zeros((cp - chans, pitch, wide), F32)

    pl.semaphore_wait(barrier, n - 1)
    early = min(EARLY, n)

    def field_copy(d, source):
        t = lax.rem(me + d, n)
        tl, tn = t // n_lon, lax.rem(t, n_lon)
        return pltpu.make_async_remote_copy(
            src_ref=nf.at[:, pl.ds(pl.multiple_of(tl * rows, rows), rows), pl.ds(pl.multiple_of(tn * wide, wide), wide)],
            dst_ref=moved.at[pl.ds(source * slots, slots)],
            send_sem=mv_send.at[d], recv_sem=mv_recv.at[d],
            device_id=(tl, tn), device_id_type=MESH,
        )

    def field_start(d, carry):
        field_copy(d, me).start()
        return carry

    lax.fori_loop(1, early, field_start, 0)
    own = pltpu.make_async_copy(
        nf.at[:, pl.ds(pl.multiple_of(lat * rows, rows), rows), pl.ds(pl.multiple_of(lon * wide, wide), wide)],
        moved.at[pl.ds(me * slots, slots)],
        own_sem,
    )
    own.start()

    def turn(r, carry):
        total, square = carry
        a = xflat[pl.ds(r, cp, stride=pitch), :]
        a = jnp.concatenate([a, jnp.zeros((kp - cp, wide), F32)], axis=0)
        t = a.T
        xt[r + 2] = t.astype(BF16)
        cols[0, pl.ds(2 * r, 1), :] = t[0:1]
        cols[0, pl.ds(2 * r + 1, 1), :] = t[1:2]
        cols[1, pl.ds(2 * r, 1), :] = t[wide - 2 : wide - 1]
        cols[1, pl.ds(2 * r + 1, 1), :] = t[wide - 1 : wide]
        parts = t.reshape(wide // 8, 8, kp)
        return total + jnp.sum(parts, axis=0), square + jnp.sum(parts * parts, axis=0)

    zero = jnp.zeros((8, kp), F32)
    total, square = lax.fori_loop(0, rows, turn, (zero, zero), unroll=4)
    stats[pl.ds(me, 1), 0:1, :] = jnp.sum(total, axis=0, keepdims=True)[None]
    stats[pl.ds(me, 1), 1:2, :] = jnp.sum(square, axis=0, keepdims=True)[None]

    def stat_copy(d, source):
        t = lax.rem(me + d, n)
        return pltpu.make_async_remote_copy(
            src_ref=stats.at[source], dst_ref=stats.at[source],
            send_sem=st_send.at[d], recv_sem=st_recv.at[d],
            device_id=(t // n_lon, lax.rem(t, n_lon)), device_id_type=MESH,
        )

    def stat_start(d, carry):
        stat_copy(d, me).start()
        return carry

    lax.fori_loop(1, n, stat_start, 0)

    north, south = lax.rem(lat + n_lat - 1, n_lat), lax.rem(lat + 1, n_lat)
    west, east = lax.rem(lon + n_lon - 1, n_lon), lax.rem(lon + 1, n_lon)
    halos = []
    for side, col_to in ((0, west), (1, east)):
        into = 1 - side
        halos.append((cols.at[side], hcol.at[into, pl.ds(8, 2 * rows)], (lat, col_to)))
        halos.append((cols.at[side, pl.ds(0, 8)], hcol.at[into, pl.ds(8 + 2 * rows, 8)], (north, col_to)))
        halos.append((cols.at[side, pl.ds(2 * rows - 8, 8)], hcol.at[into, pl.ds(0, 8)], (south, col_to)))
    halos.append((xt.at[pl.ds(2, 2)], xt.at[pl.ds(rows + 2, 2)], (north, lon)))
    halos.append((xt.at[pl.ds(rows, 2)], xt.at[pl.ds(0, 2)], (south, lon)))
    copies = [
        pltpu.make_async_remote_copy(
            src_ref=src, dst_ref=dst, send_sem=ha_send.at[i], recv_sem=ha_recv.at[i],
            device_id=where, device_id_type=MESH,
        )
        for i, (src, dst, where) in enumerate(halos)
    ]
    for copy in copies:
        copy.start()

    lax.fori_loop(early, n, field_start, 0)

    for load in loads[1:]:
        load.wait()
    for tap in range(9):
        w1s[pl.ds(tap * kp, kp), :] = jnp.concatenate(
            [w1[tap].astype(F32), jnp.zeros((kp - chans, hid), F32)], axis=0
        ).astype(BF16)

    def turn_weight(tap, carry):
        w2s[pl.ds(pl.multiple_of(tap * hid, hid), hid), :] = w2[tap].astype(F32).T.astype(BF16)
        return carry

    lax.fori_loop(0, 9, turn_weight, 0)

    def stat_wait(d, carry):
        copy = stat_copy(d, lax.rem(me - d + n, n))
        copy.wait_recv()
        return carry

    lax.fori_loop(1, n, stat_wait, 0)
    sums = jnp.sum(stats[...], axis=0)
    cells = n * rows * wide
    mean = sums[0:1] / cells
    scale = 1.0 / jnp.sqrt(sums[1:2] / cells - mean * mean + 1e-05)

    for copy in copies:
        copy.wait_recv()

    first = jnp.where(lat == 0, 0, -2)
    last = jnp.where(lat == n_lat - 1, rows - 1, rows + 1)
    tall = rows + 4
    step = en.shape[1]

    line = lax.broadcasted_iota(jnp.int32, (step, 1), 0) - 2
    inside = (line >= first) & (line <= last)
    en[...] = jnp.zeros_like(en)
    for side in range(2):
        mid = 2 if side == 0 else 0
        for j in range(2):
            en[3 * side + (j if side == 0 else j + 1), pl.ds(0, tall), :] = hcol[side, pl.ds(4 + j, tall, stride=2), :]
        at = 0 if side == 0 else wide - 1
        base = 0 if side == 0 else wide - 16
        en[3 * side + mid, pl.ds(2, rows), :] = cols[side, pl.ds(0 if side == 0 else 1, rows, stride=2), :]
        for p in (0, 1, rows + 2, rows + 3):
            en[3 * side + mid, pl.ds(p, 1), :] = xt[p, pl.ds(base, 16), :].astype(F32)[at - base : at - base + 1]
    for k in range(6):
        en[k] = jnp.where(inside, (en[k] - mean) * scale, 0.0)
    bias1 = b1[...]
    bias2 = b2[...]
    hline = lax.broadcasted_iota(jnp.int32, (rows + 2, 1), 0) - 1
    hinside = (hline >= first) & (hline <= last)
    for side in range(2):
        edge = jnp.concatenate([en[3 * side + k] for k in range(3)], axis=1).astype(BF16)
        z = [
            jnp.dot(edge, w1s[pl.ds(3 * a * kp, 3 * kp), :], preferred_element_type=F32)
            for a in range(3)
        ]
        h = z[0][0 : rows + 2] + z[1][1 : rows + 3] + z[2][2 : rows + 4] + bias1
        eh[side, pl.ds(0, rows + 2), :] = jnp.where(hinside, gelu(h), 0.0)

    spot = lax.broadcasted_iota(jnp.int32, (wide, 1), 0)

    def spread(x, left, right):
        lo = jnp.where(spot == 0, left, pltpu.roll(x, 1, 0))
        hi = jnp.where(spot == wide - 1, right, pltpu.roll(x, wide - 1, 0))
        return lo.astype(BF16), x.astype(BF16), hi.astype(BF16)

    def normal(p, carry):
        ok = (p - 2 >= first) & (p - 2 <= last)
        x = (xt[p].astype(F32) - mean) * scale
        x = jnp.where(ok, x, 0.0)
        three = spread(x, en[1, pl.ds(p, 1), :], en[4, pl.ds(p, 1), :])
        for k in range(3):
            xs[p, :, k * kp : (k + 1) * kp] = three[k]
        return carry

    lax.fori_loop(0, tall, normal, 0)

    def second(q):
        left = jnp.concatenate(
            [hs[pl.ds(q + a, 2)].reshape(2 * wide, 3 * hid) for a in range(3)], axis=1
        )
        out = jnp.dot(left, w2s[...], preferred_element_type=F32) + bias2
        for k in range(2):
            yflat[pl.ds(q + k, hid, stride=pitch), :] = out[k * wide : (k + 1) * wide].T

    def first_conv(q):
        left = jnp.concatenate(
            [xs[pl.ds(q + a, 2)].reshape(2 * wide, 3 * kp) for a in range(3)], axis=1
        )
        h = gelu(jnp.dot(left, w1s[...], preferred_element_type=F32) + bias1)
        for k in range(2):
            ok = (q + k - 1 >= first) & (q + k - 1 <= last)
            x = jnp.where(ok, h[k * wide : (k + 1) * wide], 0.0)
            three = spread(x, eh[0, pl.ds(q + k, 1), :], eh[1, pl.ds(q + k, 1), :])
            for m in range(3):
                hs[q + k, :, m * hid : (m + 1) * hid] = three[m]

    def both(b, carry):
        second(2 * b - 4)
        first_conv(2 * b)
        return carry

    first_conv(0)
    first_conv(2)
    lax.fori_loop(2, (rows + 2) // 2, both, 0)
    second(rows - 2)

    chunk = hid // 8
    for k in range(8):
        part = pl.ds(k * chunk, chunk)
        feat[part] = yf[part, 0:rows, :].astype(BF16)

    own.wait()

    def field_wait(d, carry):
        field_copy(d, lax.rem(me - d + n, n)).wait_recv()
        return carry

    lax.fori_loop(1, n, field_wait, 0)

    def take(c, carry):
        tile[c] = moved[slot[c]]
        return carry

    lax.fori_loop(0, chans, take, 0)

    def sent(d, carry):
        stat_copy(d, me).wait_send()
        field_copy(d, me).wait_send()
        return carry

    lax.fori_loop(1, n, sent, 0)
    for copy in copies:
        copy.wait_send()


def body(current, next_fields, reader_slot, first_weight, first_bias, second_weight, second_bias):
    n_lat, n_lon = lax.axis_size("lat"), lax.axis_size("lon")
    n = n_lat * n_lon
    chans, rows, wide = current.shape
    slots = next_fields.shape[0]
    hid = first_weight.shape[1]
    kp = LANES
    cp = -(-chans // 8) * 8
    pitch = 8 * (rows // 8 + 1 - rows // 8 % 2)
    step = -(-(rows + 4) // 16) * 16
    dims = (n_lat, n_lon, chans, rows, wide, slots, hid)
    vmem = pl.BlockSpec(memory_space=pltpu.VMEM)
    hbm = pl.BlockSpec(memory_space=pltpu.HBM)
    features, tile = pl.pallas_call(
        functools.partial(kernel, dims),
        out_shape=(
            jax.ShapeDtypeStruct((hid, rows, wide), BF16),
            jax.ShapeDtypeStruct((chans, rows, wide), BF16),
        ),
        in_specs=[
            hbm, hbm, hbm, hbm, hbm, hbm, hbm,
        ],
        out_specs=(vmem, vmem),
        scratch_shapes=[
            pltpu.VMEM((chans, rows, wide), BF16),
            pltpu.VMEM((9, chans, hid), BF16),
            pltpu.VMEM((9, hid, hid), BF16),
            pltpu.VMEM((1, hid), F32),
            pltpu.VMEM((1, hid), F32),
            pltpu.SMEM((chans,), jnp.int32),
            pltpu.VMEM((hid, pitch, wide), F32),
            pltpu.SemaphoreType.DMA((6,)),
            pltpu.VMEM((cp, pitch, wide), F32),
            pltpu.VMEM((rows + 4, wide, kp), BF16),
            pltpu.VMEM((2, 2 * rows, kp), F32),
            pltpu.VMEM((2, 2 * rows + 16, kp), F32),
            pltpu.VMEM((6, step, kp), F32),
            pltpu.VMEM((2, step, hid), F32),
            pltpu.VMEM((rows + 4, wide, 3 * kp), BF16),
            pltpu.VMEM((rows + 2, wide, 3 * hid), BF16),
            pltpu.VMEM((9 * kp, hid), BF16),
            pltpu.VMEM((9 * hid, hid), BF16),
            pltpu.VMEM((n, 2, kp), F32),
            pltpu.VMEM((n * slots, rows, wide), BF16),
            pltpu.SemaphoreType.DMA((n,)),
            pltpu.SemaphoreType.DMA((n,)),
            pltpu.SemaphoreType.DMA((8,)),
            pltpu.SemaphoreType.DMA((8,)),
            pltpu.SemaphoreType.DMA((n,)),
            pltpu.SemaphoreType.DMA((n,)),
            pltpu.SemaphoreType.DMA,
        ],
        compiler_params=pltpu.CompilerParams(
            collective_id=0, has_side_effects=True, vmem_limit_bytes=32 * 1024 * 1024
        ),
    )(
        *[
            pltpu.with_memory_space_constraint(x, pltpu.HBM)
            for x in (
                current, next_fields, reader_slot, first_weight.transpose(0, 2, 1),
                first_bias[None], second_weight, second_bias[None],
            )
        ]
    )
    return features, tile


def solution(mesh):
    in_specs = (P(None, "lat", "lon"), P(("lat", "lon"), None, None), P(), P(), P(), P(), P())
    out_specs = (P(None, "lat", "lon"), P(None, "lat", "lon"))
    return jax.shard_map(body, mesh=mesh, in_specs=in_specs, out_specs=out_specs, check_vma=False)
```
